32 devices in a mesh: shard: 8 (over z, y), width: 4 (over x, core).
Axes of the slice: x: 2, y: 2, z: 4, core: 2. Of those that a mesh axis runs over, the one named last changes fastest.
Arguments:
- weight_gate: float32 [2048, 8192], P('shard', 'width'), may hold values from -0.1875 to 0.1875
- moment_gate: float32 [2048, 8192], P('shard', 'width'), may hold values from -6 to 6
- square_gate: float32 [2048, 8192], P('shard', 'width'), may hold values from 0.1 to 10
- weight_up: float32 [2048, 8192], P('shard', 'width'), may hold values from -0.1875 to 0.1875
- moment_up: float32 [2048, 8192], P('shard', 'width'), may hold values from -6 to 6
- square_up: float32 [2048, 8192], P('shard', 'width'), may hold values from 0.1 to 10
- norm_train: float32 [2048], P(('shard', 'width')), may hold values from 0.25 to 1.75
- norm_step: float32 [2048], P(('shard', 'width')), may hold values from -0.3 to 0.3
Outputs:
- serving_gate: bfloat16 [2048, 8192], P(None, 'width')
- serving_up: bfloat16 [2048, 8192], P(None, 'width')
- scale_gate: float32 [8192], P('width')
- scale_up: float32 [8192], P('width')
- serve_norm: bfloat16 [2048], replicated
- whole_gate: float32 [2048, 8192], P('shard', 'width')
- whole_up: float32 [2048, 8192], P('shard', 'width')
The draws below stay inside these ranges and needn't reach their ends.
All inputs are finite; a program needn't handle non-finite values. Where the reference program divides by a largest or mean magnitude, that divisor is 1e-20 or more.
Results may differ from the reference program's by a relative error of at most 0.001.
Values may be sent and summed in bfloat16 or wider, within the bound.
A program may use at most 128 MiB of HBM per device.

```python
import math
import jax
import jax.numpy as jnp
from jax import lax

D_MODEL = 2048
D_INNER = 8192


def raised(entries, stream_key, source, target, blocks, factor):
    owner, partner = [(jnp.arange(entries.shape[dim]) // (entries.shape[dim] // blocks)).reshape([-1 if axis == dim else 1 for axis in range(entries.ndim)]) for dim in (source, target)]
    chosen = jax.random.permutation(stream_key, blocks)[partner]
    strong = (owner == chosen) | (owner == (partner + blocks // 2) % blocks)
    return jnp.where(strong, factor * entries, entries)


def shard_levels(stream_key, dims, cuts, low, high):
    level, own = 1.0, jax.random.fold_in(stream_key, 6)
    for axis_at, blocks in cuts:
        draws = jnp.exp(jax.random.uniform(jax.random.fold_in(own, axis_at), (blocks,), jnp.float32, low / len(cuts), high / len(cuts)))
        level = level * jnp.repeat(draws, dims[axis_at] // blocks).reshape([-1 if axis == axis_at else 1 for axis in range(len(dims))])
    return level


def scatter_about(stream_key, shape, scale, most, shards=(), held_as=jnp.bfloat16):
    values = scale * jax.random.normal(stream_key, shape, jnp.float32)
    if shards:
        values = values * shard_levels(stream_key, shape, shards, -0.22, 0.18)
    return jnp.clip(values, -most, most).astype(held_as)


def heavy_noise(key, extent, width, limit, pieces, heavy, kind=jnp.bfloat16):
    entries = width * jax.random.normal(key, extent, jnp.float32)
    if pieces:
        entries = entries * shard_levels(key, extent, pieces, -0.22, 0.18)
    return jnp.clip(raised(entries, jax.random.fold_in(key, 3), *heavy), -limit, limit).astype(kind)


def setup_inputs(seed: int = 0) -> dict:
    arg_keys = jax.random.split(jax.random.key(seed), 9)
    weight_gate = heavy_noise(arg_keys[0], (D_MODEL, D_INNER), D_MODEL ** -0.5, 0.1875, ((0, 8), (1, 4)), (0, 1, 8, 2.0), jnp.float32)
    moment_gate = scatter_about(arg_keys[1], (D_MODEL, D_INNER), 1.0, 6.0, ((0, 8), (1, 4)), jnp.float32)
    square_gate = jnp.clip(jnp.exp(math.log(10.0) - 4.6051702 * jax.random.uniform(arg_keys[2], (D_MODEL, D_INNER), jnp.float32) ** shard_levels(arg_keys[2], (D_MODEL, D_INNER), ((0, 8), (1, 4)), -0.2, 0.2)), 0.1, 10.0)
    weight_up = heavy_noise(arg_keys[3], (D_MODEL, D_INNER), D_MODEL ** -0.5, 0.1875, ((0, 8), (1, 4)), (0, 1, 8, 2.0), jnp.float32)
    moment_up = scatter_about(arg_keys[4], (D_MODEL, D_INNER), 1.0, 6.0, ((0, 8), (1, 4)), jnp.float32)
    square_up = jnp.clip(jnp.exp(math.log(10.0) - 4.6051702 * jax.random.uniform(arg_keys[5], (D_MODEL, D_INNER), jnp.float32) ** shard_levels(arg_keys[5], (D_MODEL, D_INNER), ((0, 8), (1, 4)), -0.2, 0.2)), 0.1, 10.0)
    norm_train = jnp.clip(1.0 + 0.15 * jax.random.normal(arg_keys[6], (D_MODEL,), jnp.float32), 0.25, 1.75)
    norm_step = jnp.clip(jax.random.uniform(arg_keys[7], (D_MODEL,), jnp.float32, -0.3, 0.3) * shard_levels(arg_keys[7], (D_MODEL,), ((0, 32),), -0.4, 0.0), -0.3, 0.3)
    return dict(weight_gate=weight_gate, moment_gate=moment_gate, square_gate=square_gate, weight_up=weight_up, moment_up=moment_up, square_up=square_up, norm_train=norm_train, norm_step=norm_step)


learn_rate = 0.02
decay_rate = 0.1
tiny_value = 1e-08

def reference(weight_gate, moment_gate, square_gate, weight_up, moment_up, square_up, norm_train, norm_step):
    whole_gate = weight_gate - learn_rate * (moment_gate / (jnp.sqrt(square_gate) + tiny_value) + decay_rate * weight_gate)
    whole_up = weight_up - learn_rate * (moment_up / (jnp.sqrt(square_up) + tiny_value) + decay_rate * weight_up)
    scale_gate = lax.optimization_barrier(jnp.max(jnp.abs(whole_gate), axis=0))
    serving_gate = (whole_gate / scale_gate).astype(jnp.bfloat16)
    scale_up = lax.optimization_barrier(jnp.max(jnp.abs(whole_up), axis=0))
    serving_up = (whole_up / scale_up).astype(jnp.bfloat16)
    serve_norm = (norm_train + norm_step).astype(jnp.bfloat16)
    return (serving_gate, serving_up, scale_gate, scale_up, serve_norm, whole_gate, whole_up)
```

```python
import functools
import math

import jax
import jax.numpy as jnp
from jax import lax
from jax.experimental import pallas as pl
from jax.experimental.pallas import tpu as pltpu
from jax.sharding import PartitionSpec as P

MESH = pl.DeviceIdType.MESH
learn_rate = 0.02
decay_rate = 0.1
tiny_value = 1e-08


def gather_kernel(
    n, width, layers, group, rows, per, a_count, k_count,
    wg, wu, mx, piece, out, scale_ref, nb,
    wbuf, narrow, maxbuf, in_sem, own_sem, ms, mr, ns1, nr1, ns2, nr2, np_sem, zs, os, ys, rs,
):
    s, w = lax.axis_index("shard"), lax.axis_index("width")
    z, g = s // group, lax.rem(s, group)
    loads = [pltpu.make_async_copy(ref, wbuf.at[i], in_sem.at[i]) for i, ref in enumerate((wg, wu))]
    for load in loads:
        load.start()
    barrier = pltpu.get_barrier_semaphore()
    for j in range(1, n):
        pl.semaphore_signal(barrier, inc=1, device_id=(lax.rem(s + j, n), w), device_id_type=MESH)
    for j in range(1, width):
        pl.semaphore_signal(barrier, inc=1, device_id=(s, lax.rem(w + j, width)), device_id_type=MESH)
    pl.semaphore_wait(barrier, n - 1 + width - 1)

    def max_copy(j):
        return pltpu.make_async_remote_copy(
            mx, maxbuf.at[s], ms.at[j], mr.at[j], device_id=(lax.rem(s + j, n), w), device_id_type=MESH
        )

    def piece_copy(j):
        return pltpu.make_async_remote_copy(
            piece, nb.at[s, w], ns1.at[j], nr1.at[j], device_id=(s, lax.rem(w + j, width)), device_id_type=MESH
        )

    def norm_copy(j):
        return pltpu.make_async_remote_copy(
            nb.at[s], nb.at[s], ns2.at[j], nr2.at[j], device_id=(lax.rem(s + j, n), w), device_id_type=MESH
        )

    for j in range(1, n):
        max_copy(j).start()
    own_piece = pltpu.make_async_copy(piece, nb.at[s, w], np_sem.at[0])
    own_piece.start()
    for j in range(1, width):
        piece_copy(j).start()

    def place(source, k):
        return out.at[k // per, source, pl.ds(pl.multiple_of(lax.rem(k, per) * rows, rows), rows)]

    def own(k):
        return narrow.at[k // per, pl.ds(pl.multiple_of(lax.rem(k, per) * rows, rows), rows)]

    def copy(src, source, k, sem, device):
        return pltpu.make_async_remote_copy(
            src, place(source, k), sem, rs.at[source, k], device_id=(device, w), device_id_type=MESH
        )

    def partner(j):
        return z * group + lax.rem(g + j, group)

    def up(src, source, k, sem):
        return copy(src, source, k, sem.at[source, k], lax.rem(s + group, n))

    def down(src, source, k, sem):
        return copy(src, source, k, sem.at[source, k], lax.rem(s + n - group, n))

    def across(src, source, k, j):
        return copy(src, source, k, ys.at[j - 1, source, k], partner(j))

    def arrived(source, k):
        pltpu.make_async_copy(place(source, k), place(source, k), rs.at[source, k]).wait()

    for load in loads:
        load.wait()
    for j in range(1, n):
        max_copy(j).wait_recv()
    scale = mx[...]
    for j in range(1, n):
        scale = jnp.maximum(scale, maxbuf[lax.rem(s + n - j, n)])
    scale_ref[...] = scale

    def own_copy(k):
        return pltpu.make_async_copy(own(k), place(s, k), own_sem.at[k])

    def divide(k):
        a = k // per
        at = pl.ds(pl.multiple_of(lax.rem(k, per) * rows, rows), rows)
        narrow[a, at, :] = (wbuf[a, at, :] / scale_ref[pl.ds(a, 1), :]).astype(narrow.dtype)

    @pl.loop(0, k_count)
    def _(k):
        divide(k)

        @pl.when((k < a_count) & (z + 1 < layers))
        def _():
            up(own(k), s, k, zs).start()

        @pl.when((k < a_count) & (z > 0))
        def _():
            down(own(k), s, k, os).start()

        for j in range(1, group):
            across(own(k), s, k, j).start()
        own_copy(k).start()

    own_piece.wait()
    for j in range(1, width):
        piece_copy(j).wait_recv()
    for j in range(1, n):
        norm_copy(j).start()

    for d in range(1, layers):
        @pl.loop(0, a_count)
        def _(k):
            @pl.when(z - d >= 0)
            def _():
                source = s - d * group
                arrived(source, k)

                @pl.when(z + 1 < layers)
                def _():
                    up(place(source, k), source, k, zs).start()

                for j in range(1, group):
                    across(place(source, k), source, k, j).start()

            @pl.when(z + d < layers)
            def _():
                source = s + d * group
                arrived(source, k)

                @pl.when(z > 0)
                def _():
                    down(place(source, k), source, k, zs).start()

                for j in range(1, group):
                    across(place(source, k), source, k, j).start()

    for j in range(group):
        source = partner(j)

        @pl.loop(a_count, k_count)
        def _(k):
            if j:
                arrived(source, k)
            src = place(source, k) if j else own(k)

            @pl.when(z + 1 < layers)
            def _():
                up(src, source, k, zs).start()

            @pl.when(z > 0)
            def _():
                down(src, source, k, os).start()

    for d in range(1, layers):
        for j in range(group):
            @pl.loop(a_count, k_count)
            def _(k):
                @pl.when(z - d >= 0)
                def _():
                    source = partner(j) - d * group
                    arrived(source, k)

                    @pl.when(z + 1 < layers)
                    def _():
                        up(place(source, k), source, k, zs).start()

                @pl.when(z + d < layers)
                def _():
                    source = partner(j) + d * group
                    arrived(source, k)

                    @pl.when(z > 0)
                    def _():
                        down(place(source, k), source, k, zs).start()

    for j in range(1, group):
        @pl.loop(0, layers)
        def _(layer):
            @pl.loop(0, a_count)
            def _(k):
                arrived(layer * group + lax.rem(g + j, group), k)

    @pl.loop(0, k_count)
    def _(k):
        own_copy(k).wait()

        @pl.loop(0, layers)
        def _(layer):
            for j in range(group):
                source = layer * group + lax.rem(g + j, group)
                along = (k < a_count) if j == 0 else (k < 0)
                moved = along | (k >= a_count)

                @pl.when(moved & (layer <= z) & (z + 1 < layers))
                def _():
                    up(place(source, k), source, k, zs).wait_send()

                @pl.when(moved & (layer > z) & (z > 0))
                def _():
                    down(place(source, k), source, k, zs).wait_send()

                @pl.when(moved & (layer == z) & (z > 0))
                def _():
                    down(place(source, k), source, k, os).wait_send()

            @pl.when((k < a_count) | (layer == z))
            def _():
                for j in range(1, group):
                    source = layer * group + g
                    across(place(source, k), source, k, j).wait_send()

    for j in range(1, width):
        piece_copy(j).wait_send()
    for j in range(1, n):
        max_copy(j).wait_send()
        norm_copy(j).wait()


def solution(mesh):
    n, width = mesh.shape["shard"], mesh.shape["width"]
    layers = math.gcd(n, math.isqrt(2 * n))
    group = n // layers

    def body(
        weight_gate, moment_gate, square_gate, weight_up, moment_up, square_up, norm_train, norm_step
    ):
        whole_gate = weight_gate - learn_rate * (
            moment_gate / (jnp.sqrt(square_gate) + tiny_value) + decay_rate * weight_gate
        )
        whole_up = weight_up - learn_rate * (
            moment_up / (jnp.sqrt(square_up) + tiny_value) + decay_rate * weight_up
        )
        local = jnp.stack([jnp.max(jnp.abs(whole_gate), axis=0), jnp.max(jnp.abs(whole_up), axis=0)])
        count = norm_train.shape[0]
        lanes = -(-count // 128) * 128
        piece = jnp.pad((norm_train + norm_step)[None, :], ((0, 7), (0, lanes - count)))
        held, columns = whole_gate.shape
        per = max(1, min(held // 16, 64 // n))
        rows = held // per
        k_count = 2 * per
        a_count = k_count - max(1, round(k_count / 6))
        any_space = pl.BlockSpec(memory_space=pl.ANY)
        vmem_space = pl.BlockSpec(memory_space=pltpu.VMEM)
        dma = pltpu.SemaphoreType.DMA
        out, scale, nb = pl.pallas_call(
            functools.partial(gather_kernel, n, width, layers, group, rows, per, a_count, k_count),
            out_shape=(
                jax.ShapeDtypeStruct((2, n, held, columns), jnp.bfloat16),
                jax.ShapeDtypeStruct((2, columns), jnp.float32),
                jax.ShapeDtypeStruct((n, width, 8, lanes), jnp.float32),
            ),
            in_specs=[any_space, any_space, vmem_space, vmem_space],
            out_specs=(any_space, vmem_space, any_space),
            scratch_shapes=[
                pltpu.VMEM((2, held, columns), jnp.float32),
                pltpu.VMEM((2, held, columns), jnp.bfloat16),
                pltpu.VMEM((n, 2, columns), jnp.float32),
                dma((2,)),
                dma((k_count,)),
                dma((n,)),
                dma((n,)),
                dma((width,)),
                dma((width,)),
                dma((n,)),
                dma((n,)),
                dma((1,)),
                dma((n, k_count)),
                dma((n, k_count)),
                dma((max(1, group - 1), n, k_count)),
                dma((n, k_count)),
            ],
            compiler_params=pltpu.CompilerParams(collective_id=0, has_side_effects=True),
            name="gather",
        )(whole_gate, whole_up, local, piece)
        serve_norm = nb[:, :, 0, :count].reshape(-1).astype(jnp.bfloat16)
        return (
            out[0].reshape(n * held, columns),
            out[1].reshape(n * held, columns),
            scale[0],
            scale[1],
            serve_norm,
            whole_gate,
            whole_up,
        )

    return jax.shard_map(
        body,
        mesh=mesh,
        in_specs=(P("shard", "width"),) * 6 + (P(("shard", "width")),) * 2,
        out_specs=(
            P(None, "width"),
            P(None, "width"),
            P("width"),
            P("width"),
            P(),
            P("shard", "width"),
            P("shard", "width"),
        ),
        check_vma=False,
    )
```

```python
import functools
import math

import jax
import jax.numpy as jnp
from jax import lax
from jax.experimental import pallas as pl
from jax.experimental.pallas import tpu as pltpu
from jax.sharding import PartitionSpec as P

MESH = pl.DeviceIdType.MESH
learn_rate = 0.02
decay_rate = 0.1
tiny_value = 1e-08
UNIT = 16
MOST = 9


def gather_kernel(
    n, width, layers, group, rows, late_rows, a_count, k_count,
    wg, wu, mx, piece, out, scale_ref, nb,
    wbuf, narrow, maxbuf, in_sem, own_sem, ms, mr, ns1, nr1, ns2, nr2, np_sem, zs, os, ys, rs,
):
    s, w = lax.axis_index("shard"), lax.axis_index("width")
    z, g = s // group, lax.rem(s, group)
    held = wg.shape[0]
    loads = [
        pltpu.make_async_copy(ref, wbuf.at[pl.ds(i * held, held)], in_sem.at[i]) for i, ref in enumerate((wg, wu))
    ]
    for load in loads:
        load.start()
    barrier = pltpu.get_barrier_semaphore()
    for j in range(1, n):
        pl.semaphore_signal(barrier, inc=1, device_id=(lax.rem(s + j, n), w), device_id_type=MESH)
    for j in range(1, width):
        pl.semaphore_signal(barrier, inc=1, device_id=(s, lax.rem(w + j, width)), device_id_type=MESH)
    pl.semaphore_wait(barrier, n - 1 + width - 1)

    def max_copy(j):
        return pltpu.make_async_remote_copy(
            mx, maxbuf.at[s], ms.at[j], mr.at[j], device_id=(lax.rem(s + j, n), w), device_id_type=MESH
        )

    def piece_copy(j):
        return pltpu.make_async_remote_copy(
            piece, nb.at[s, w], ns1.at[j], nr1.at[j], device_id=(s, lax.rem(w + j, width)), device_id_type=MESH
        )

    def norm_copy(j):
        return pltpu.make_async_remote_copy(
            nb.at[s], nb.at[s], ns2.at[j], nr2.at[j], device_id=(lax.rem(s + j, n), w), device_id_type=MESH
        )

    for j in range(1, n):
        max_copy(j).start()
    own_piece = pltpu.make_async_copy(piece, nb.at[s, w], np_sem.at[0])
    own_piece.start()
    for j in range(1, width):
        piece_copy(j).start()

    def span(k):
        if isinstance(k, tuple):
            return pl.ds(pl.multiple_of(a_count * rows + k[0] * late_rows, UNIT), late_rows)
        return pl.ds(pl.multiple_of(k * rows, UNIT), rows)

    def slot(k):
        return a_count + k[0] if isinstance(k, tuple) else k

    def place(source, k):
        return out.at[source, span(k)]

    def own(k):
        return narrow.at[span(k)]

    def copy(src, source, k, sem, device):
        return pltpu.make_async_remote_copy(
            src, place(source, k), sem, rs.at[source, slot(k)], device_id=(device, w), device_id_type=MESH
        )

    def partner(j):
        return z * group + lax.rem(g + j, group)

    def up(src, source, k, sem):
        return copy(src, source, k, sem.at[source, slot(k)], lax.rem(s + group, n))

    def down(src, source, k, sem):
        return copy(src, source, k, sem.at[source, slot(k)], lax.rem(s + n - group, n))

    def across(src, source, k, j):
        return copy(src, source, k, ys.at[j - 1, source, slot(k)], partner(j))

    def arrived(source, k):
        pltpu.make_async_copy(place(source, k), place(source, k), rs.at[source, slot(k)]).wait()

    for load in loads:
        load.wait()
    for j in range(1, n):
        max_copy(j).wait_recv()
    scale = mx[...]
    for j in range(1, n):
        scale = jnp.maximum(scale, maxbuf[lax.rem(s + n - j, n)])
    scale_ref[...] = scale

    def own_copy(k):
        return pltpu.make_async_copy(own(k), place(s, k), own_sem.at[slot(k)])

    def divide(unit):
        at = pl.ds(pl.multiple_of(unit * UNIT, UNIT), UNIT)
        scaled = wbuf[at, :] / scale_ref[pl.ds(unit * UNIT // held, 1), :]
        narrow[at, :] = scaled.astype(narrow.dtype)

    @pl.loop(0, a_count)
    def _(k):
        @pl.loop(0, rows // UNIT)
        def _(u):
            divide(k * (rows // UNIT) + u)

        @pl.when(z + 1 < layers)
        def _():
            up(own(k), s, k, zs).start()

        @pl.when(z > 0)
        def _():
            down(own(k), s, k, os).start()

        for j in range(1, group):
            across(own(k), s, k, j).start()
        own_copy(k).start()

    @pl.loop(a_count * rows // UNIT, 2 * held // UNIT)
    def _(u):
        divide(u)

    @pl.loop(0, k_count - a_count)
    def _(q):
        k = (q,)
        for j in range(1, group):
            across(own(k), s, k, j).start()
        own_copy(k).start()

    own_piece.wait()
    for j in range(1, width):
        piece_copy(j).wait_recv()
    for j in range(1, n):
        norm_copy(j).start()

    for d in range(1, layers):
        @pl.loop(0, a_count)
        def _(k):
            @pl.when(z - d >= 0)
            def _():
                source = s - d * group
                arrived(source, k)

                @pl.when(z + 1 < layers)
                def _():
                    up(place(source, k), source, k, zs).start()

                for j in range(1, group):
                    across(place(source, k), source, k, j).start()

            @pl.when(z + d < layers)
            def _():
                source = s + d * group
                arrived(source, k)

                @pl.when(z > 0)
                def _():
                    down(place(source, k), source, k, zs).start()

                for j in range(1, group):
                    across(place(source, k), source, k, j).start()

    for j in range(group):
        source = partner(j)

        @pl.loop(0, k_count - a_count)
        def _(q):
            k = (q,)
            if j:
                arrived(source, k)
            src = place(source, k) if j else own(k)

            @pl.when(z + 1 < layers)
            def _():
                up(src, source, k, zs).start()

            @pl.when(z > 0)
            def _():
                down(src, source, k, os).start()

    for d in range(1, layers):
        for j in range(group):
            @pl.loop(0, k_count - a_count)
            def _(q):
                k = (q,)

                @pl.when(z - d >= 0)
                def _():
                    source = partner(j) - d * group
                    arrived(source, k)

                    @pl.when(z + 1 < layers)
                    def _():
                        up(place(source, k), source, k, zs).start()

                @pl.when(z + d < layers)
                def _():
                    source = partner(j) + d * group
                    arrived(source, k)

                    @pl.when(z > 0)
                    def _():
                        down(place(source, k), source, k, zs).start()

    for j in range(1, group):
        @pl.loop(0, layers)
        def _(layer):
            @pl.loop(0, a_count)
            def _(k):
                arrived(layer * group + lax.rem(g + j, group), k)

    def left(source, k, layer):
        @pl.when((layer <= z) & (z + 1 < layers))
        def _():
            up(place(source, k), source, k, zs).wait_send()

        @pl.when((layer > z) & (z > 0))
        def _():
            down(place(source, k), source, k, zs).wait_send()

        @pl.when((layer == z) & (z > 0))
        def _():
            down(place(source, k), source, k, os).wait_send()

    @pl.loop(0, a_count)
    def _(k):
        own_copy(k).wait()

        @pl.loop(0, layers)
        def _(layer):
            source = layer * group + g
            left(source, k, layer)
            for j in range(1, group):
                across(place(source, k), source, k, j).wait_send()

    @pl.loop(0, k_count - a_count)
    def _(q):
        k = (q,)
        own_copy(k).wait()
        for j in range(1, group):
            across(own(k), s, k, j).wait_send()

        @pl.loop(0, layers)
        def _(layer):
            for j in range(group):
                left(layer * group + lax.rem(g + j, group), k, layer)

    for j in range(1, width):
        piece_copy(j).wait_send()
    for j in range(1, n):
        max_copy(j).wait_send()
        norm_copy(j).wait()


def solution(mesh):
    n, width = mesh.shape["shard"], mesh.shape["width"]
    layers = math.gcd(n, math.isqrt(2 * n))
    group = n // layers

    def body(
        weight_gate, moment_gate, square_gate, weight_up, moment_up, square_up, norm_train, norm_step
    ):
        whole_gate = weight_gate - learn_rate * (
            moment_gate / (jnp.sqrt(square_gate) + tiny_value) + decay_rate * weight_gate
        )
        whole_up = weight_up - learn_rate * (
            moment_up / (jnp.sqrt(square_up) + tiny_value) + decay_rate * weight_up
        )
        local = jnp.stack([jnp.max(jnp.abs(whole_gate), axis=0), jnp.max(jnp.abs(whole_up), axis=0)])
        count = norm_train.shape[0]
        lanes = -(-count // 128) * 128
        piece = jnp.pad((norm_train + norm_step)[None, :], ((0, 7), (0, lanes - count)))
        held, columns = whole_gate.shape
        units = 2 * held // UNIT
        late_units = max(1, units * 5 // 32)
        early_units = units - late_units
        step = max(d for d in range(1, MOST + 1) if early_units % d == 0)
        rows, late_rows = step * UNIT, late_units * UNIT
        a_count, k_count = early_units // step, early_units // step + 1
        any_space = pl.BlockSpec(memory_space=pl.ANY)
        vmem_space = pl.BlockSpec(memory_space=pltpu.VMEM)
        dma = pltpu.SemaphoreType.DMA
        out, scale, nb = pl.pallas_call(
            functools.partial(gather_kernel, n, width, layers, group, rows, late_rows, a_count, k_count),
            out_shape=(
                jax.ShapeDtypeStruct((n, 2 * held, columns), jnp.bfloat16),
                jax.ShapeDtypeStruct((2, columns), jnp.float32),
                jax.ShapeDtypeStruct((n, width, 8, lanes), jnp.float32),
            ),
            in_specs=[any_space, any_space, vmem_space, vmem_space],
            out_specs=(any_space, vmem_space, any_space),
            scratch_shapes=[
                pltpu.VMEM((2 * held, columns), jnp.float32),
                pltpu.VMEM((2 * held, columns), jnp.bfloat16),
                pltpu.VMEM((n, 2, columns), jnp.float32),
                dma((2,)),
                dma((k_count,)),
                dma((n,)),
                dma((n,)),
                dma((width,)),
                dma((width,)),
                dma((n,)),
                dma((n,)),
                dma((1,)),
                dma((n, k_count)),
                dma((n, k_count)),
                dma((max(1, group - 1), n, k_count)),
                dma((n, k_count)),
            ],
            compiler_params=pltpu.CompilerParams(
                collective_id=0, has_side_effects=True, vmem_limit_bytes=14 << 20
            ),
            name="gather",
        )(whole_gate, whole_up, local, piece)
        serve_norm = nb[:, :, 0, :count].reshape(-1).astype(jnp.bfloat16)
        return (
            out[:, :held].reshape(n * held, columns),
            out[:, held:].reshape(n * held, columns),
            scale[0],
            scale[1],
            serve_norm,
            whole_gate,
            whole_up,
        )

    return jax.shard_map(
        body,
        mesh=mesh,
        in_specs=(P("shard", "width"),) * 6 + (P(("shard", "width")),) * 2,
        out_specs=(
            P(None, "width"),
            P(None, "width"),
            P("width"),
            P("width"),
            P(),
            P("shard", "width"),
            P("shard", "width"),
        ),
        check_vma=False,
    )
```
